32 devices in a mesh: pq: 2 (over x), rs: 16 (over z, y, core).
Axes of the slice: x: 2, y: 2, z: 4, core: 2. Of those that a mesh axis runs over, the one named last changes fastest.
Arguments:
- integrals: bfloat16 [128, 1152, 1152], P('pq', 'rs'), may hold values from -6 to 6
- coeff: bfloat16 [1152, 896], P('rs', 'pq'), may hold values from -0.1875 to 0.1875
Outputs:
- half_mo: bfloat16 [128, 896, 896], P('pq', 'rs')
The draws below stay inside these ranges and needn't reach their ends.
All inputs are finite; a program needn't handle non-finite values.
Results may differ from the reference program's by a relative error of at most 0.0049.
Values may be sent and summed in bfloat16 or wider, within the bound.
A program may use at most 128 MiB of HBM per device.

```python
import jax
import jax.numpy as jnp
from jax import lax

NBASIS = 1152
NORB = 896
PAIRS = 128


def block_scale(own_key, dims, split, smallest, top_value):
    factor_of, own = 1.0, jax.random.fold_in(own_key, 6)
    for dim, parts in split:
        steps = jnp.exp(jax.random.uniform(jax.random.fold_in(own, dim), (parts,), jnp.float32, smallest / len(split), top_value / len(split)))
        factor_of = factor_of * jnp.repeat(steps, dims[dim] // parts).reshape([-1 if axis == dim else 1 for axis in range(len(dims))])
    return factor_of


def noise(own_key, shape, width, bound, cuts=(), kind=jnp.bfloat16):
    drawn = width * jax.random.normal(own_key, shape, jnp.float32)
    if cuts:
        drawn = drawn * block_scale(own_key, shape, cuts, -0.22, 0.18)
    return jnp.clip(drawn, -bound, bound).astype(kind)


def setup_inputs(seed: int = 0) -> dict:
    splits = jax.random.split(jax.random.key(seed), 3)
    return {
        "integrals": noise(splits[0], (PAIRS, NBASIS, NBASIS), 1.0, 6.0, ((0, 2), (1, 16))),
        "coeff": noise(splits[1], (NBASIS, NORB), NBASIS ** -0.5, 0.1875, ((0, 16), (1, 2))),
    }


def reference(integrals, coeff):
    pairs = integrals.shape[0]
    flat = integrals.reshape(pairs * NBASIS, NBASIS)
    first = jnp.dot(flat, coeff, preferred_element_type=jnp.float32).astype(jnp.bfloat16)
    first = first.reshape(pairs, NBASIS, NORB)

    def one_row(block):
        return jnp.dot(block.T, coeff, preferred_element_type=jnp.float32).astype(jnp.bfloat16)

    return lax.map(one_row, first)
```

```python
import functools
import math

import jax
import jax.numpy as jnp
from jax import lax
from jax.experimental import pallas as pl
from jax.experimental.pallas import tpu as pltpu
from jax.sharding import PartitionSpec as P

MESH = pl.DeviceIdType.MESH


def second_half(received, panel):
    return jnp.einsum("prl,rk->plk", received, panel, preferred_element_type=jnp.float32).astype(
        jnp.bfloat16
    )


def plain(integrals, panel):
    pair_rows, block_rows, nbasis = integrals.shape
    flat = integrals.reshape(pair_rows * block_rows, nbasis)
    first = jnp.dot(flat, panel, preferred_element_type=jnp.float32).astype(jnp.bfloat16)
    first = first.reshape(pair_rows, block_rows, panel.shape[1])
    return second_half(lax.all_to_all(first, "rs", split_axis=2, concat_axis=1, tiled=True), panel)


def fused_kernel(n, group, x_ref, c_ref, o_ref, tiles, send, recv, stage, load_sem, send_sem, recv_sem, own_sem, out_sem):
    me = lax.axis_index("rs")
    groups = send.shape[0]
    rows = send.shape[2]
    width = stage.shape[2]
    nbasis = tiles.shape[3]
    half = n // 2
    far = lax.rem(me // half + 1, 2) * half
    near = (me // half) * half

    def load(g):
        return pltpu.make_async_copy(x_ref.at[pl.ds(g * group, group)], tiles.at[g % 2], load_sem.at[g % 2])

    def store(g):
        return pltpu.make_async_copy(stage.at[g % 2], o_ref.at[pl.ds(g * group, group)], out_sem.at[g % 2])

    def partner(i):
        if i < half:
            return far + lax.rem(me + i, half)
        return near + lax.rem(me + i - half + 1, half)

    def remote(g, i):
        to = partner(i)
        return pltpu.make_async_remote_copy(
            src_ref=send.at[g, to],
            dst_ref=recv.at[g, me],
            send_sem=send_sem.at[g, i],
            recv_sem=recv_sem.at[g, i],
            device_id={"rs": to},
            device_id_type=MESH,
        )

    def own(g):
        return pltpu.make_async_copy(send.at[g, me], recv.at[g, me], own_sem.at[g])

    load(0).start()
    barrier = pltpu.get_barrier_semaphore()
    for i in range(1, n):
        pl.semaphore_signal(barrier, inc=1, device_id={"rs": lax.rem(me + i, n)}, device_id_type=MESH)
    pl.semaphore_wait(barrier, n - 1)

    step = 4
    for g in range(groups):
        if g + 1 < groups:
            load(g + 1).start()
        load(g).wait()
        for q in range(group // step):
            block = tiles[g % 2, q * step : (q + 1) * step].reshape(step * rows, nbasis)
            first = jnp.dot(block, c_ref[...], preferred_element_type=jnp.float32)
            for j in range(step):
                slot = q * step + j
                piece = first[j * rows : (j + 1) * rows].astype(jnp.bfloat16)
                for d in range(n):
                    send[g, d, :, slot * width : (slot + 1) * width] = piece[:, d * width : (d + 1) * width]
        for i in range(n - 1):
            remote(g, i).start()
        own(g).start()

    for g in range(groups):
        own(g).wait()
        for i in range(n - 1):
            remote(g, i).wait()
        lhs = recv[g].reshape(n * rows, group * width)
        out = lax.dot_general(lhs, c_ref[...], (((0,), (0,)), ((), ())), preferred_element_type=jnp.float32)
        if g >= 2:
            store(g - 2).wait()
        for j in range(group):
            stage[g % 2, j] = out[j * width : (j + 1) * width].astype(jnp.bfloat16)
        store(g).start()
    for g in range(max(groups - 2, 0), groups):
        store(g).wait()


def fused(n, group, integrals, panel):
    pair_rows, rows, nbasis = integrals.shape
    norb = panel.shape[1]
    width = norb // n
    groups = pair_rows // group
    flops = 2 * pair_rows * rows * nbasis * norb + 2 * pair_rows * width * n * rows * norb
    sent = 2 * pair_rows * rows * norb
    return pl.pallas_call(
        functools.partial(fused_kernel, n, group),
        out_shape=jax.ShapeDtypeStruct((pair_rows, width, norb), jnp.bfloat16),
        in_specs=[pl.BlockSpec(memory_space=pl.ANY), pl.BlockSpec(memory_space=pltpu.VMEM)],
        out_specs=pl.BlockSpec(memory_space=pl.ANY),
        scratch_shapes=[
            pltpu.VMEM((2, group, rows, nbasis), jnp.bfloat16),
            pltpu.VMEM((groups, n, rows, group * width), jnp.bfloat16),
            pltpu.VMEM((groups, n, rows, group * width), jnp.bfloat16),
            pltpu.VMEM((2, group, width, norb), jnp.bfloat16),
            pltpu.SemaphoreType.DMA((2,)),
            pltpu.SemaphoreType.DMA((groups, n)),
            pltpu.SemaphoreType.DMA((groups, n)),
            pltpu.SemaphoreType.DMA((groups,)),
            pltpu.SemaphoreType.DMA((2,)),
        ],
        compiler_params=pltpu.CompilerParams(
            collective_id=0, has_side_effects=True, vmem_limit_bytes=60 * 2**20
        ),
        cost_estimate=pl.CostEstimate(flops=flops, bytes_accessed=4 * sent, transcendentals=0),
    )(integrals, panel)


def on_device(n, integrals, coeff):
    pair_rows, rows, nbasis = integrals.shape
    strip = lax.all_gather(coeff, "pq", axis=1, tiled=True)
    panel = lax.all_gather(strip, "rs", axis=0, tiled=True)
    width = panel.shape[1] // n
    group = math.lcm(4, 128 // math.gcd(width, 128))
    if rows % 8 or width % 8 or n % 2 or pair_rows % group or group * width > 2048:
        return plain(integrals, panel)
    return fused(n, group, integrals, panel)


def solution(mesh):
    placed = (P("pq", "rs", None), P("rs", "pq"))
    return jax.shard_map(
        functools.partial(on_device, mesh.shape["rs"]),
        mesh=mesh,
        in_specs=placed,
        out_specs=P("pq", "rs", None),
        check_vma=False,
    )
```

```python
import functools
import math

import jax
import jax.numpy as jnp
from jax import lax
from jax.experimental import pallas as pl
from jax.experimental.pallas import tpu as pltpu
from jax.sharding import PartitionSpec as P

MESH = pl.DeviceIdType.MESH


def second_half(received, panel):
    return jnp.einsum("prl,rk->plk", received, panel, preferred_element_type=jnp.float32).astype(
        jnp.bfloat16
    )


def plain(integrals, panel):
    pair_rows, block_rows, nbasis = integrals.shape
    flat = integrals.reshape(pair_rows * block_rows, nbasis)
    first = jnp.dot(flat, panel, preferred_element_type=jnp.float32).astype(jnp.bfloat16)
    first = first.reshape(pair_rows, block_rows, panel.shape[1])
    return second_half(lax.all_to_all(first, "rs", split_axis=2, concat_axis=1, tiled=True), panel)


def fused_kernel(n, group, x_ref, c_ref, o_ref, tiles, parts, panel, send, recv, stage, load_sem, send_sem, recv_sem, own_sem, out_sem, hop_sem, part_sem, local_sem):
    me = lax.axis_index("rs")
    col = lax.axis_index("pq")
    groups = send.shape[0]
    rows = send.shape[2]
    width = stage.shape[2]
    nbasis = tiles.shape[3]
    half = n // 2
    far_side = lax.rem(me // half + 1, 2)
    near_side = me // half
    far = far_side * half
    near = near_side * half
    lines = n // 4
    core = lax.rem(me, 2)
    y = lax.rem(me // 2, 2)
    z = me // 4
    col_too = 1 - col

    def spot(at_z, at_y, at_core):
        return at_z * 4 + at_y * 2 + at_core

    def load(g):
        return pltpu.make_async_copy(x_ref.at[pl.ds(g * group, group)], tiles.at[g % 2], load_sem.at[g % 2])

    def store(g):
        return pltpu.make_async_copy(stage.at[g % 2], o_ref.at[pl.ds(g * group, group)], out_sem.at[g % 2])

    def partner(i):
        if i < half:
            return far + lax.rem(me + i, half)
        return near + lax.rem(me + i - half + 1, half)

    def remote(g, i):
        to = partner(i)
        return pltpu.make_async_remote_copy(
            src_ref=send.at[g, to],
            dst_ref=recv.at[g, me],
            send_sem=send_sem.at[g, i],
            recv_sem=recv_sem.at[g, i],
            device_id={"rs": to},
            device_id_type=MESH,
        )

    def own(g):
        return pltpu.make_async_copy(send.at[g, me], recv.at[g, me], own_sem.at[g])

    load(0).start()
    local = pltpu.make_async_copy(c_ref, parts.at[col, me], local_sem)
    local.start()
    barrier = pltpu.get_barrier_semaphore()
    for i in range(1, n):
        pl.semaphore_signal(barrier, inc=1, device_id={"rs": lax.rem(me + i, n)}, device_id_type=MESH)
    pl.semaphore_signal(barrier, inc=1, device_id={"pq": col_too}, device_id_type=MESH)
    pl.semaphore_wait(barrier, n)

    hops = []

    def pass_on(q, r, to, src=None):
        copy = pltpu.make_async_remote_copy(
            src_ref=parts.at[q, r] if src is None else src,
            dst_ref=parts.at[q, r],
            send_sem=hop_sem.at[len(hops)],
            recv_sem=part_sem.at[q, r],
            device_id=to,
            device_id_type=MESH,
        )
        copy.start()
        hops.append(copy)

    def arrived(q, r):
        pltpu.make_async_remote_copy(
            src_ref=parts.at[q, r],
            dst_ref=parts.at[q, r],
            send_sem=hop_sem.at[0],
            recv_sem=part_sem.at[q, r],
            device_id={"pq": col_too},
            device_id_type=MESH,
        ).wait_recv()

    across_y = {"rs": spot(z, 1 - y, core)}
    across_x = {"pq": col_too}
    across_core = {"rs": spot(z, y, 1 - core)}
    for k in range(1, lines):
        pass_on(col, me, {"rs": spot(lax.rem(z + k, lines), y, core)}, c_ref)
    for k in range(lines):
        r = spot(lax.rem(z + lines - k, lines), y, core)
        if k:
            arrived(col, r)
        src = None if k else c_ref
        pass_on(col, r, across_y, src)
        pass_on(col, r, across_x, src)
        pass_on(col, r, across_core, src)
    for k in range(lines):
        at_z = lax.rem(z + lines - k, lines)
        mine, other = spot(at_z, y, core), spot(at_z, 1 - y, core)
        arrived(col_too, mine)
        arrived(col, other)
        if k % 2:
            pass_on(col, other, across_x)
        else:
            pass_on(col_too, mine, across_y)
        pass_on(col_too, mine, across_core)
        pass_on(col, other, across_core)
    for k in range(lines):
        other = spot(lax.rem(z + lines - k, lines), 1 - y, core)
        arrived(col_too, other)
        pass_on(col_too, other, across_core)
    for k in range(lines):
        for q in (col, col_too):
            for at_y in (0, 1):
                arrived(q, spot(k, at_y, 1 - core))
    local.wait()

    step = 4
    for g in range(groups):
        if g + 1 < groups:
            load(g + 1).start()
        load(g).wait()
        for side in (0, 1):
            weights = parts[near_side if side else far_side].reshape(nbasis, half * width)
            base = near if side else far
            for q in range(group // step):
                block = tiles[g % 2, q * step : (q + 1) * step].reshape(step * rows, nbasis)
                first = jnp.dot(block, weights, preferred_element_type=jnp.float32)
                for j in range(step):
                    slot = q * step + j
                    piece = first[j * rows : (j + 1) * rows].astype(jnp.bfloat16)
                    for d in range(half):
                        send[g, base + d, :, slot * width : (slot + 1) * width] = piece[:, d * width : (d + 1) * width]
            for i in range(half, n - 1) if side else range(half):
                remote(g, i).start()
        own(g).start()

    for q in (0, 1):
        panel[:, q * half * width : (q + 1) * half * width] = parts[q].reshape(nbasis, half * width)
    for copy in hops:
        copy.wait_send()

    contract = (((0,), (0,)), ((), ()))
    for g in range(groups):
        own(g).wait()
        if g + 1 < groups:
            for i in range(n - 1):
                remote(g, i).wait()
            lhs = recv[g].reshape(n * rows, group * width)
            out = lax.dot_general(lhs, panel[...], contract, preferred_element_type=jnp.float32)
        else:
            out = 0.0
            for side in (1, 0):
                base = near if side else far
                for i in range(half, n - 1) if side else range(half):
                    remote(g, i).wait()
                lhs = recv[g, pl.ds(base, half)].reshape(half * rows, group * width)
                part = panel[pl.ds(pl.multiple_of(base * rows, 16), half * rows)]
                out += lax.dot_general(lhs, part, contract, preferred_element_type=jnp.float32)
        if g >= 2:
            store(g - 2).wait()
        for j in range(group):
            stage[g % 2, j] = out[j * width : (j + 1) * width].astype(jnp.bfloat16)
        store(g).start()
    for g in range(max(groups - 2, 0), groups):
        store(g).wait()


def fused(n, group, integrals, coeff):
    pair_rows, rows, nbasis = integrals.shape
    columns = coeff.shape[1]
    norb = 2 * columns
    width = norb // n
    groups = pair_rows // group
    flops = 2 * pair_rows * rows * nbasis * norb + 2 * pair_rows * width * n * rows * norb
    sent = 2 * pair_rows * rows * norb
    return pl.pallas_call(
        functools.partial(fused_kernel, n, group),
        out_shape=jax.ShapeDtypeStruct((pair_rows, width, norb), jnp.bfloat16),
        in_specs=[pl.BlockSpec(memory_space=pl.ANY), pl.BlockSpec(memory_space=pltpu.VMEM)],
        out_specs=pl.BlockSpec(memory_space=pl.ANY),
        scratch_shapes=[
            pltpu.VMEM((2, group, rows, nbasis), jnp.bfloat16),
            pltpu.VMEM((2, n, rows, columns), jnp.bfloat16),
            pltpu.VMEM((nbasis, norb), jnp.bfloat16),
            pltpu.VMEM((groups, n, rows, group * width), jnp.bfloat16),
            pltpu.VMEM((groups, n, rows, group * width), jnp.bfloat16),
            pltpu.VMEM((2, group, width, norb), jnp.bfloat16),
            pltpu.SemaphoreType.DMA((2,)),
            pltpu.SemaphoreType.DMA((groups, n)),
            pltpu.SemaphoreType.DMA((groups, n)),
            pltpu.SemaphoreType.DMA((groups,)),
            pltpu.SemaphoreType.DMA((2,)),
            pltpu.SemaphoreType.DMA((2 * n,)),
            pltpu.SemaphoreType.DMA((2, n)),
            pltpu.SemaphoreType.DMA,
        ],
        compiler_params=pltpu.CompilerParams(
            collective_id=0, has_side_effects=True, vmem_limit_bytes=60 * 2**20
        ),
        cost_estimate=pl.CostEstimate(flops=flops, bytes_accessed=4 * sent, transcendentals=0),
    )(integrals, coeff)


def on_device(n, splits, integrals, coeff):
    pair_rows, rows, nbasis = integrals.shape
    norb = coeff.shape[1] * splits
    width = norb // n
    group = math.lcm(4, 128 // math.gcd(width, 128))
    aligned = rows % 8 == 0 and width % 8 == 0 and pair_rows % group == 0 and n * rows % 32 == 0
    if splits == 2 and n % 4 == 0 and aligned and group * width <= 2048:
        return fused(n, group, integrals, coeff)
    strip = lax.all_gather(coeff, "pq", axis=1, tiled=True)
    return plain(integrals, lax.all_gather(strip, "rs", axis=0, tiled=True))


def solution(mesh):
    placed = (P("pq", "rs", None), P("rs", "pq"))
    return jax.shard_map(
        functools.partial(on_device, mesh.shape["rs"], mesh.shape["pq"]),
        mesh=mesh,
        in_specs=placed,
        out_specs=P("pq", "rs", None),
        check_vma=False,
    )
```

```python
import functools
import math

import jax
import jax.numpy as jnp
from jax import lax
from jax.experimental import pallas as pl
from jax.experimental.pallas import tpu as pltpu
from jax.sharding import PartitionSpec as P

MESH = pl.DeviceIdType.MESH


def second_half(received, panel):
    return jnp.einsum("prl,rk->plk", received, panel, preferred_element_type=jnp.float32).astype(
        jnp.bfloat16
    )


def plain(integrals, panel):
    pair_rows, block_rows, nbasis = integrals.shape
    flat = integrals.reshape(pair_rows * block_rows, nbasis)
    first = jnp.dot(flat, panel, preferred_element_type=jnp.float32).astype(jnp.bfloat16)
    first = first.reshape(pair_rows, block_rows, panel.shape[1])
    return second_half(lax.all_to_all(first, "rs", split_axis=2, concat_axis=1, tiled=True), panel)


def fused_kernel(n, group, x_ref, c_ref, o_ref, tiles, parts, panel, send, recv, stage, load_sem, send_sem, recv_sem, own_sem, out_sem, hop_sem, part_sem, local_sem):
    me = lax.axis_index("rs")
    col = lax.axis_index("pq")
    groups = send.shape[0]
    rows = send.shape[2]
    width = stage.shape[2]
    nbasis = tiles.shape[3]
    half = n // 2
    far_side = lax.rem(me // half + 1, 2)
    near_side = me // half
    far = far_side * half
    near = near_side * half
    lines = n // 4
    core = lax.rem(me, 2)
    y = lax.rem(me // 2, 2)
    z = me // 4
    col_too = 1 - col

    def spot(at_z, at_y, at_core):
        return at_z * 4 + at_y * 2 + at_core

    def load(g):
        return pltpu.make_async_copy(x_ref.at[pl.ds(g * group, group)], tiles.at[g % 2], load_sem.at[g % 2])

    def store(g):
        return pltpu.make_async_copy(stage.at[g % 2], o_ref.at[pl.ds(g * group, group)], out_sem.at[g % 2])

    def partner(i):
        if i < half:
            pair = lax.rem(lax.rem(me, half) // 2 + i // 2, half // 2)
            return far + pair * 2 + lax.rem(me + i, 2)
        return near + lax.rem(me + i - half + 1, half)

    cuts = 3 if rows % 24 == 0 else 1
    short = rows // cuts

    def remote(g, i, cut=None):
        to = partner(i)
        first_cut = g == 0 and i < half
        some = pl.ds((cut or 0) * short, short) if first_cut else pl.ds(0, rows)
        sem = groups + cut - 1 if first_cut and cut else g
        return pltpu.make_async_remote_copy(
            src_ref=send.at[g, to, some],
            dst_ref=recv.at[g, me, some],
            send_sem=send_sem.at[sem, i],
            recv_sem=recv_sem.at[sem, i],
            device_id={"rs": to},
            device_id_type=MESH,
        )

    def own(g):
        return pltpu.make_async_copy(send.at[g, me], recv.at[g, me], own_sem.at[g])

    load(0).start()
    local = pltpu.make_async_copy(c_ref, parts.at[col, me], local_sem)
    local.start()
    barrier = pltpu.get_barrier_semaphore()
    for i in range(1, n):
        pl.semaphore_signal(barrier, inc=1, device_id={"rs": lax.rem(me + i, n)}, device_id_type=MESH)
    pl.semaphore_signal(barrier, inc=1, device_id={"pq": col_too}, device_id_type=MESH)
    pl.semaphore_wait(barrier, n)

    hops = []

    def pass_on(q, r, to, src=None):
        copy = pltpu.make_async_remote_copy(
            src_ref=parts.at[q, r] if src is None else src,
            dst_ref=parts.at[q, r],
            send_sem=hop_sem.at[len(hops)],
            recv_sem=part_sem.at[q, r],
            device_id=to,
            device_id_type=MESH,
        )
        copy.start()
        hops.append(copy)

    def arrived(q, r):
        pltpu.make_async_remote_copy(
            src_ref=parts.at[q, r],
            dst_ref=parts.at[q, r],
            send_sem=hop_sem.at[0],
            recv_sem=part_sem.at[q, r],
            device_id={"pq": col_too},
            device_id_type=MESH,
        ).wait_recv()

    across_y = {"rs": spot(z, 1 - y, core)}
    across_x = {"pq": col_too}
    across_core = {"rs": spot(z, y, 1 - core)}
    for k in range(1, lines):
        pass_on(col, me, {"rs": spot(lax.rem(z + k, lines), y, core)}, c_ref)
    def along(k):
        return lax.rem(z + lines - k, lines)

    for k in range(lines + 2):
        if k < lines:
            r = spot(along(k), y, core)
            if k:
                arrived(col, r)
            src = None if k else c_ref
            pass_on(col, r, across_y, src)
            pass_on(col, r, across_x, src)
            pass_on(col, r, across_core, src)
        if 0 <= k - 1 < lines:
            mine, other = spot(along(k - 1), y, core), spot(along(k - 1), 1 - y, core)
            arrived(col_too, mine)
            arrived(col, other)
            if (k - 1) % 2:
                pass_on(col, other, across_x)
            else:
                pass_on(col_too, mine, across_y)
            pass_on(col_too, mine, across_core)
            pass_on(col, other, across_core)
        if 0 <= k - 2:
            other = spot(along(k - 2), 1 - y, core)
            arrived(col_too, other)
            pass_on(col_too, other, across_core)
    local.wait()

    def arrived_from_core(q):
        for k in range(lines):
            for at_y in (0, 1):
                arrived(q, spot(k, at_y, 1 - core))

    step = 4
    for g in range(groups):
        if g + 1 < groups:
            load(g + 1).start()
        load(g).wait()
        for side in (0, 1):
            if g == 0:
                arrived_from_core(near_side if side else far_side)
            weights = parts[near_side if side else far_side].reshape(nbasis, half * width)
            base = near if side else far
            if g == 0 and side == 0:
                for cut in range(cuts):
                    block = tiles[0, :, cut * short : (cut + 1) * short].reshape(group * short, nbasis)
                    first = jnp.dot(block, weights, preferred_element_type=jnp.float32)
                    for slot in range(group):
                        piece = first[slot * short : (slot + 1) * short].astype(jnp.bfloat16)
                        for d in range(half):
                            send[0, base + d, cut * short : (cut + 1) * short, slot * width : (slot + 1) * width] = piece[:, d * width : (d + 1) * width]
                    for i in range(half):
                        remote(0, i, cut).start()
                continue
            for q in range(group // step):
                block = tiles[g % 2, q * step : (q + 1) * step].reshape(step * rows, nbasis)
                first = jnp.dot(block, weights, preferred_element_type=jnp.float32)
                for j in range(step):
                    slot = q * step + j
                    piece = first[j * rows : (j + 1) * rows].astype(jnp.bfloat16)
                    for d in range(half):
                        send[g, base + d, :, slot * width : (slot + 1) * width] = piece[:, d * width : (d + 1) * width]
            for i in range(half, n - 1) if side else range(half):
                remote(g, i).start()
        own(g).start()

    for q in (0, 1):
        panel[:, q * half * width : (q + 1) * half * width] = parts[q].reshape(nbasis, half * width)
    for copy in hops:
        copy.wait_send()

    contract = (((0,), (0,)), ((), ()))
    for g in range(groups):
        own(g).wait()
        if g + 1 < groups:
            for i in range(n - 1):
                for cut in range(cuts if g == 0 and i < half else 1):
                    remote(g, i, cut).wait()
            lhs = recv[g].reshape(n * rows, group * width)
            out = lax.dot_general(lhs, panel[...], contract, preferred_element_type=jnp.float32)
        else:
            for i in range(half, n - 1):
                remote(g, i).wait()
            chunks = [(near, half)]
            for a in range(half // 2):
                pair = lax.rem(lax.rem(me, half) // 2 + half // 2 - a, half // 2)
                chunks.append((far + 2 * pair, 2))
            out = 0.0
            for at, (base, count) in enumerate(chunks):
                if at:
                    remote(g, 2 * at - 2).wait()
                    remote(g, 2 * at - 1).wait()
                lhs = recv[g, pl.ds(base, count)].reshape(count * rows, group * width)
                part = panel[pl.ds(pl.multiple_of(base * rows, 16), count * rows)]
                out += lax.dot_general(lhs, part, contract, preferred_element_type=jnp.float32)
        if g >= 2:
            store(g - 2).wait()
        for j in range(group):
            stage[g % 2, j] = out[j * width : (j + 1) * width].astype(jnp.bfloat16)
        store(g).start()
    for g in range(max(groups - 2, 0), groups):
        store(g).wait()


def fused(n, group, integrals, coeff):
    pair_rows, rows, nbasis = integrals.shape
    columns = coeff.shape[1]
    norb = 2 * columns
    width = norb // n
    groups = pair_rows // group
    flops = 2 * pair_rows * rows * nbasis * norb + 2 * pair_rows * width * n * rows * norb
    sent = 2 * pair_rows * rows * norb
    return pl.pallas_call(
        functools.partial(fused_kernel, n, group),
        out_shape=jax.ShapeDtypeStruct((pair_rows, width, norb), jnp.bfloat16),
        in_specs=[pl.BlockSpec(memory_space=pl.ANY), pl.BlockSpec(memory_space=pltpu.VMEM)],
        out_specs=pl.BlockSpec(memory_space=pl.ANY),
        scratch_shapes=[
            pltpu.VMEM((2, group, rows, nbasis), jnp.bfloat16),
            pltpu.VMEM((2, n, rows, columns), jnp.bfloat16),
            pltpu.VMEM((nbasis, norb), jnp.bfloat16),
            pltpu.VMEM((groups, n, rows, group * width), jnp.bfloat16),
            pltpu.VMEM((groups, n, rows, group * width), jnp.bfloat16),
            pltpu.VMEM((2, group, width, norb), jnp.bfloat16),
            pltpu.SemaphoreType.DMA((2,)),
            pltpu.SemaphoreType.DMA((groups + 2, n)),
            pltpu.SemaphoreType.DMA((groups + 2, n)),
            pltpu.SemaphoreType.DMA((groups,)),
            pltpu.SemaphoreType.DMA((2,)),
            pltpu.SemaphoreType.DMA((2 * n,)),
            pltpu.SemaphoreType.DMA((2, n)),
            pltpu.SemaphoreType.DMA,
        ],
        compiler_params=pltpu.CompilerParams(
            collective_id=0, has_side_effects=True, vmem_limit_bytes=60 * 2**20
        ),
        cost_estimate=pl.CostEstimate(flops=flops, bytes_accessed=4 * sent, transcendentals=0),
    )(integrals, coeff)


def on_device(n, splits, integrals, coeff):
    pair_rows, rows, nbasis = integrals.shape
    norb = coeff.shape[1] * splits
    width = norb // n
    group = math.lcm(4, 128 // math.gcd(width, 128))
    aligned = rows % 8 == 0 and width % 8 == 0 and pair_rows % group == 0 and pair_rows >= 2 * group
    if splits == 2 and n % 4 == 0 and aligned and group * width <= 2048:
        return fused(n, group, integrals, coeff)
    strip = lax.all_gather(coeff, "pq", axis=1, tiled=True)
    return plain(integrals, lax.all_gather(strip, "rs", axis=0, tiled=True))


def solution(mesh):
    placed = (P("pq", "rs", None), P("rs", "pq"))
    return jax.shard_map(
        functools.partial(on_device, mesh.shape["rs"], mesh.shape["pq"]),
        mesh=mesh,
        in_specs=placed,
        out_specs=P("pq", "rs", None),
        check_vma=False,
    )
```
